8 devices in a mesh: tp: 4 (over z, y, x), dp: 2 (over core).
Axes of the slice: x: 2, y: 2, z: 1, core: 2. Of those that a mesh axis runs over, the one named last changes fastest.
Arguments:
- hidden: bfloat16 [2, 1024, 1024], P('dp')
- gain: float32 [1024], replicated
- embedding: bfloat16 [250112, 1024], P('tp')
- targets: int32 [2, 1024], P('dp')
- weights: float32 [2, 1024], P('dp')
Outputs:
- output 1: float32 [], replicated
- output 2: bfloat16 [2, 1024, 1024], P('dp')
- output 3: float32 [250112, 1024], P('tp')
- output 4: float32 [1024], replicated
All inputs are finite; a program needn't handle non-finite values.
Results may differ from the reference program's by a relative error of at most 0.001.
Values sent between devices are 32-bit elements.
A program may use at most 1.5 GiB of HBM per device.

```python
import math
import jax
import jax.numpy as jnp
from jax import lax

D_MODEL = 1024
VOCAB_SIZE = 250112
BATCH_ROWS = 2
SEQ_LEN = 1024
DATA_SHARDS = 2
TOKEN_COUNT = BATCH_ROWS * SEQ_LEN
ROW_BLOCK = math.gcd(TOKEN_COUNT, 128)
LN_EPS = 1e-6
Z_COEF = 1e-4
EMB_SCALE = 2.0
TARGET_PULL = 2.0


def setup_inputs(seed: int = 0) -> dict:
    key = jax.random.key(seed)
    key_cap, key_len, key_tgt, key_emb, key_noise, key_gain = jax.random.split(key, 6)
    quarters = jax.random.randint(key_cap, (DATA_SHARDS,), 1, 5)
    seq_cap = jnp.repeat(quarters, BATCH_ROWS // DATA_SHARDS) * SEQ_LEN // 4
    lengths = jax.random.randint(key_len, (BATCH_ROWS,), 1, seq_cap + 1).at[0].set(SEQ_LEN)
    weights = (jnp.arange(SEQ_LEN)[None, :] < lengths[:, None]).astype(jnp.float32)
    targets = jax.random.randint(key_tgt, (BATCH_ROWS, SEQ_LEN), 0, VOCAB_SIZE)
    emb_f32 = jax.random.normal(key_emb, (VOCAB_SIZE, D_MODEL), jnp.float32) * (EMB_SCALE / math.sqrt(D_MODEL))
    embedding = emb_f32.astype(jnp.bfloat16)
    noise = jax.random.normal(key_noise, (BATCH_ROWS, SEQ_LEN, D_MODEL), jnp.float32)
    hidden = (noise + TARGET_PULL * embedding.astype(jnp.float32)[targets]).astype(jnp.bfloat16)
    gain = 1.0 + 0.2 * jax.random.normal(key_gain, (D_MODEL,), jnp.float32)
    return {'hidden': hidden, 'gain': gain, 'embedding': embedding, 'targets': targets, 'weights': weights}


def reference(hidden, gain, embedding, targets, weights):
    block_count = TOKEN_COUNT // ROW_BLOCK
    tok_scale = weights / weights.sum()
    blocks = (hidden.reshape(block_count, ROW_BLOCK, D_MODEL), targets.reshape(block_count, ROW_BLOCK), tok_scale.reshape(block_count, ROW_BLOCK))
    vocab_ids = jnp.arange(VOCAB_SIZE)

    def block_step(carry, block):
        d_emb, d_gain, loss = carry
        rows, row_targets, row_scale = block
        hid_f32 = rows.astype(jnp.float32)
        centered = hid_f32 - hid_f32.mean(-1, keepdims=True)
        inv_std = lax.rsqrt((centered * centered).mean(-1, keepdims=True) + LN_EPS)
        x_hat = centered * inv_std
        normed = (x_hat * gain).astype(jnp.bfloat16)
        logits = jnp.dot(normed, embedding.T, preferred_element_type=jnp.float32)
        peak = logits.max(-1, keepdims=True)
        log_z = peak[:, 0] + jnp.log(jnp.exp(logits - peak).sum(-1))
        is_target = vocab_ids[None, :] == row_targets[:, None]
        tgt_logit = jnp.where(is_target, logits, 0.0).sum(-1)
        loss = loss + (row_scale * (log_z - tgt_logit + Z_COEF * log_z * log_z)).sum()
        soft_probs = jnp.exp(logits - log_z[:, None])
        grad_logits = ((soft_probs * (1.0 + 2.0 * Z_COEF * log_z)[:, None] - is_target.astype(jnp.float32)) * row_scale[:, None]).astype(jnp.bfloat16)
        d_normed = jnp.dot(grad_logits, embedding, preferred_element_type=jnp.float32)
        d_emb = d_emb + jnp.dot(grad_logits.T, normed, preferred_element_type=jnp.float32)
        d_gain = d_gain + (d_normed * x_hat).sum(0)
        d_xhat = d_normed * gain
        d_rows = inv_std * (d_xhat - d_xhat.mean(-1, keepdims=True) - x_hat * (d_xhat * x_hat).mean(-1, keepdims=True))
        return (d_emb, d_gain, loss), d_rows.astype(jnp.bfloat16)

    start_carry = (jnp.zeros((VOCAB_SIZE, D_MODEL), jnp.float32), jnp.zeros((D_MODEL,), jnp.float32), jnp.zeros((), jnp.float32))
    (d_emb, d_gain, loss), d_rows = lax.scan(block_step, start_carry, blocks)
    return loss, d_rows.reshape(BATCH_ROWS, SEQ_LEN, D_MODEL), d_emb, d_gain
```

```python
import functools

import jax
import jax.numpy as jnp
from jax import lax
from jax.experimental import pallas as pl
from jax.experimental.pallas import tpu as pltpu
from jax.sharding import PartitionSpec as P

LN_EPS = 1e-6
Z_COEF = 1e-4
TILE = 1024
SUB = 256
BLOCK = 256
LANES = 128
NEG = -3.0e38
F32 = jnp.float32
BF16 = jnp.bfloat16


def _logits_body(rows, tokens, emb_ref, yft_ref, log_ref, m_ref, s_ref):
    sub = min(rows, SUB)
    for r in range(0, rows, sub):
        log_ref[r:r + sub, :] = jnp.dot(emb_ref[r:r + sub, :], yft_ref[...], preferred_element_type=F32)
        for c in range(0, tokens, LANES):
            cols = slice(c, c + LANES)
            tops = [log_ref[r + k:r + k + 8, cols] for k in range(0, sub, 8)]
            while len(tops) > 1:
                tops = [jnp.maximum(a, b) for a, b in zip(tops[::2], tops[1::2])] + ([tops[-1]] if len(tops) % 2 else [])
            old = m_ref[:, cols]
            new = jnp.maximum(old, tops[0])
            sums = [jnp.exp(log_ref[r + k:r + k + 8, cols] - new) for k in range(0, sub, 8)]
            while len(sums) > 1:
                sums = [a + b for a, b in zip(sums[::2], sums[1::2])] + ([sums[-1]] if len(sums) % 2 else [])
            s_ref[:, cols] = s_ref[:, cols] * jnp.exp(old - new) + sums[0]
            m_ref[:, cols] = new


def _logits_kernel(tokens, last, rest, emb_ref, yft_ref, log_ref, m_ref, s_ref):
    j = pl.program_id(0)

    @pl.when(j == 0)
    def _():
        m_ref[...] = jnp.full_like(m_ref, NEG)
        s_ref[...] = jnp.zeros_like(s_ref)

    @pl.when(j != last)
    def _():
        _logits_body(TILE, tokens, emb_ref, yft_ref, log_ref, m_ref, s_ref)

    @pl.when(j == last)
    def _():
        _logits_body(rest, tokens, emb_ref, yft_ref, log_ref, m_ref, s_ref)


def _grad_body(rows, tokens, first_row, with_dyf, log_ref, emb_ref, yf_ref, vec_ref, tgt_ref, de_ref, tl_ref, dyf_ref, g_ref):
    sub = min(rows, SUB)
    for r in range(0, rows, sub):
        for c in range(0, tokens, LANES):
            cols = slice(c, c + LANES)
            log_z, scale, weight = vec_ref[0:1, cols], vec_ref[1:2, cols], vec_ref[2:3, cols]
            ids = tgt_ref[0:1, cols] - (first_row + r)
            hit_sum = jnp.zeros((8, LANES), F32)
            for k in range(0, sub, 64):
                logit = log_ref[r + k:r + k + 64, cols]
                hit = (lax.broadcasted_iota(jnp.int32, (64, LANES), 0) + k) == ids
                grad = jnp.exp(logit - log_z) * scale - jnp.where(hit, weight, 0.0)
                g_ref[r + k:r + k + 64, cols] = grad.astype(BF16)
                found = jnp.where(hit, logit, 0.0)
                for q in range(0, 64, 8):
                    hit_sum = hit_sum + found[q:q + 8, :]
            tl_ref[:, cols] += hit_sum
        de_ref[r:r + sub, :] = jnp.dot(g_ref[r:r + sub, :], yf_ref[...], preferred_element_type=F32)
    if with_dyf:
        dyf_ref[...] += lax.dot_general(emb_ref[0:rows, :], g_ref[0:rows, :], (((0,), (0,)), ((), ())), preferred_element_type=F32)


def _grad_kernel(tokens, last, rest, with_dyf, aliased, base_ref, *refs):
    if with_dyf:
        log_ref, emb_ref, yf_ref, vec_ref, tgt_ref, *refs = refs
    else:
        log_ref, yf_ref, vec_ref, tgt_ref, *refs = refs
        emb_ref = None
    if aliased:
        refs = refs[1:]
    if with_dyf:
        de_ref, tl_ref, dyf_ref, g_ref = refs
    else:
        de_ref, tl_ref, g_ref = refs
        dyf_ref = None
    tile = base_ref[0] + pl.program_id(0)

    @pl.when(pl.program_id(0) == 0)
    def _():
        tl_ref[...] = jnp.zeros_like(tl_ref)
        if with_dyf:
            dyf_ref[...] = jnp.zeros_like(dyf_ref)

    body = functools.partial(_grad_body, tokens=tokens, first_row=tile * TILE, with_dyf=with_dyf, log_ref=log_ref, emb_ref=emb_ref,
                             yf_ref=yf_ref, vec_ref=vec_ref, tgt_ref=tgt_ref, de_ref=de_ref, tl_ref=tl_ref, dyf_ref=dyf_ref, g_ref=g_ref)
    pl.when(tile != last)(lambda: body(TILE))
    pl.when(tile == last)(lambda: body(rest))


def solution(mesh):
    def local_step(hidden, gain, emb_rows, targets, weights):
        vocab_rows, width = emb_rows.shape
        seq = hidden.shape[1]
        n_tiles = pl.cdiv(vocab_rows, TILE)
        n_tiles += n_tiles % 2
        half = n_tiles // 2
        last, rest = vocab_rows // TILE, vocab_rows % TILE
        me = lax.axis_index('dp')
        swap = functools.partial(lax.ppermute, axis_name='dp', perm=[(0, 1), (1, 0)])

        hid_f32 = hidden[0].astype(F32)
        centered = hid_f32 - hid_f32.mean(-1, keepdims=True)
        inv_std = lax.rsqrt((centered * centered).mean(-1, keepdims=True) + LN_EPS)
        x_hat = centered * inv_std

        def both(mine, other):
            return jnp.where(me == 0, mine, other), jnp.where(me == 0, other, mine)

        x0, x1 = both(x_hat, swap(x_hat))
        t0, t1 = both(targets[0], swap(targets[0]))
        w0, w1 = both(weights[0], swap(weights[0]))
        n0 = w0.sum().astype(jnp.int32)
        n1 = w1.sum().astype(jnp.int32)
        blocks0, blocks1 = (n0 + BLOCK - 1) // BLOCK, (n1 + BLOCK - 1) // BLOCK
        start1 = blocks0 * BLOCK
        w_total = w0.sum() + w1.sum()

        def pack(a, b):
            full = jnp.concatenate([a, jnp.zeros_like(a)], 0)
            return lax.dynamic_update_slice(full, b, (start1,) + (0,) * (a.ndim - 1))

        yf = pack((x0 * gain).astype(BF16), (x1 * gain).astype(BF16))
        tok_scale = pack(w0, w1) / w_total
        local_ids = pack(t0, t1) - lax.axis_index('tp') * vocab_rows

        def branch(tokens):
            def run(yf, tok_scale, local_ids, emb_rows):
                yf, tok_scale, local_ids = yf[:tokens], tok_scale[:tokens], local_ids[:tokens]
                params = pltpu.CompilerParams(dimension_semantics=('arbitrary',), vmem_limit_bytes=62 * 2**20)
                logits, m, s = pl.pallas_call(
                    functools.partial(_logits_kernel, tokens, last, rest),
                    grid=(pl.cdiv(vocab_rows, TILE),),
                    in_specs=[pl.BlockSpec((TILE, width), lambda j: (j, 0)),
                              pl.BlockSpec((width, tokens), lambda j: (0, 0), pipeline_mode=pl.Buffered(1))],
                    out_specs=[pl.BlockSpec((TILE, tokens), lambda j: (j, 0)),
                               pl.BlockSpec((8, tokens), lambda j: (0, 0)),
                               pl.BlockSpec((8, tokens), lambda j: (0, 0))],
                    out_shape=[jax.ShapeDtypeStruct((vocab_rows, tokens), F32),
                               jax.ShapeDtypeStruct((8, tokens), F32),
                               jax.ShapeDtypeStruct((8, tokens), F32)],
                    compiler_params=params, name='logits')(emb_rows, yf.T)
                peak = lax.pmax(m.max(0), 'tp')
                exp_sum = lax.psum((s * jnp.exp(m - peak[None])).sum(0), 'tp')
                log_z = peak + jnp.log(exp_sum)
                vec = jnp.stack([log_z, (1.0 + 2.0 * Z_COEF * log_z) * tok_scale, tok_scale] + [tok_scale] * 5)
                tgt = jnp.broadcast_to(local_ids[None], (8, tokens))

                def grads(base, with_dyf, d_emb):
                    row = lambda i, b: (b[0] + i, 0)
                    fixed = lambda i, b: (0, 0)
                    one = pl.Buffered(1)
                    ins = [(logits, pl.BlockSpec((TILE, tokens), row))]
                    if with_dyf:
                        ins.append((emb_rows, pl.BlockSpec((TILE, width), row)))
                    ins += [(yf, pl.BlockSpec((tokens, width), fixed, pipeline_mode=one)),
                            (vec, pl.BlockSpec((8, tokens), fixed)), (tgt, pl.BlockSpec((8, tokens), fixed))]
                    alias = {}
                    if d_emb is not None:
                        alias = {len(ins) + 1: 0}
                        ins.append((d_emb, pl.BlockSpec(memory_space=pl.ANY)))
                    outs = [(jax.ShapeDtypeStruct((vocab_rows, width), F32), pl.BlockSpec((TILE, width), row)),
                            (jax.ShapeDtypeStruct((8, tokens), F32), pl.BlockSpec((8, tokens), fixed))]
                    if with_dyf:
                        outs.append((jax.ShapeDtypeStruct((width, tokens), F32), pl.BlockSpec((width, tokens), fixed, pipeline_mode=one)))
                    flops = 2 * half * TILE * tokens * width * (2 if with_dyf else 1)
                    return pl.pallas_call(
                        functools.partial(_grad_kernel, tokens, last, rest, with_dyf, d_emb is not None),
                        grid_spec=pltpu.PrefetchScalarGridSpec(
                            num_scalar_prefetch=1, grid=(half,), in_specs=[b for _, b in ins], out_specs=[b for _, b in outs],
                            scratch_shapes=[pltpu.VMEM((TILE, tokens), BF16)]),
                        out_shape=[a for a, _ in outs], input_output_aliases=alias, compiler_params=params,
                        cost_estimate=pl.CostEstimate(flops=flops, bytes_accessed=half * TILE * (tokens + 2 * width) * 4, transcendentals=0),
                        name='grads_both' if with_dyf else 'grads_emb')(base, *[a for a, _ in ins])

                base_a = jnp.full((1,), half, jnp.int32) * me
                base_b = jnp.full((1,), half, jnp.int32) * (1 - me)
                d_emb, tl_a, dyf_t = grads(base_a, True, None)
                d_part = dyf_t.T
                d0 = d_part[:seq]
                d1 = lax.dynamic_slice(jnp.pad(d_part, ((0, 2 * seq - tokens), (0, 0))), (start1, 0), (seq, width))
                mine, others = jnp.where(me == 0, d0, d1), jnp.where(me == 0, d1, d0)
                d_normed = lax.psum(mine + swap(others), 'tp')
                d_emb, tl_b = grads(base_b, False, d_emb)[:2]
                tgt_sum = (tok_scale * (tl_a + tl_b).sum(0)).sum()
                z_sum = (tok_scale * (log_z + Z_COEF * log_z * log_z)).sum()
                return d_emb, d_normed, 0.5 * (0.25 * z_sum - tgt_sum)
            return run

        sizes = range(5 * BLOCK, 2 * seq + 1, BLOCK)
        which = jnp.clip(blocks0 + blocks1 - 5, 0, len(sizes) - 1)
        d_emb, d_normed, loss_part = lax.switch(which, [branch(n) for n in sizes], yf, tok_scale, local_ids, emb_rows)

        d_normed = jnp.where(weights[0][:, None] > 0, d_normed, 0.0)
        sums = jnp.concatenate([0.25 * (d_normed * x_hat).sum(0), jnp.full((LANES,), loss_part)])
        sums = lax.psum(sums, ('tp', 'dp'))
        d_rows = d_normed * gain
        d_hidden = inv_std * (d_rows - d_rows.mean(-1, keepdims=True) - x_hat * (d_rows * x_hat).mean(-1, keepdims=True))
        return sums[width], d_hidden.astype(BF16)[None], d_emb, sums[:width]

    return jax.shard_map(local_step, mesh=mesh,
                         in_specs=(P('dp', None, None), P(None), P('tp', None), P('dp', None), P('dp', None)),
                         out_specs=(P(), P('dp', None, None), P('tp', None), P(None)),
                         check_vma=False)
```

```python
import functools

import jax
import jax.numpy as jnp
from jax import lax
from jax.experimental import pallas as pl
from jax.experimental.pallas import tpu as pltpu
from jax.sharding import PartitionSpec as P

LN_EPS = 1e-6
Z_COEF = 1e-4
TILE = 1024
SUB = 256
BLOCK = 256
LANES = 128
STAT_SUB = 128
SPAN = 512
NEG = -3.0e38
SENT = {5: (15, 15), 6: (17, 8), 7: (18, 9), 8: (19, 8)}
F32 = jnp.float32
BF16 = jnp.bfloat16


def _dot(a, b):
    return jnp.dot(a, b, preferred_element_type=F32)


def _tree(op, parts):
    while len(parts) > 1:
        parts = [op(a, b) for a, b in zip(parts[::2], parts[1::2])] + ([parts[-1]] if len(parts) % 2 else [])
    return parts[0]


def _stats(r, sub, cols, first_row, log_ref, tgt_ref, m_ref, s_ref, tl_ref):
    ids = tgt_ref[:, cols] - (first_row + r) - lax.broadcasted_iota(jnp.int32, (8, LANES), 0)
    tl_ref[:, cols] += _tree(jnp.add, [jnp.where(ids == k, log_ref[r + k:r + k + 8, cols], 0.0) for k in range(0, sub, 8)])
    old = m_ref[:, cols]
    new = jnp.maximum(old, _tree(jnp.maximum, [log_ref[r + k:r + k + 8, cols] for k in range(0, sub, 8)]))
    total = _tree(jnp.add, [jnp.exp(log_ref[r + k:r + k + 8, cols] - new) for k in range(0, sub, 8)])
    s_ref[:, cols] = s_ref[:, cols] * jnp.exp(old - new) + total
    m_ref[:, cols] = new


def _columns(tokens):
    return [slice(c, c + LANES) for c in range(0, tokens, LANES)]


def _logits_body(rows, tokens, first_row, emb_ref, yft_ref, tgt_ref, log_ref, m_ref, s_ref, tl_ref):
    sub = min(rows, STAT_SUB)
    for r in range(0, rows + sub, sub):
        if r < rows:
            log_ref[r:r + sub, :] = _dot(emb_ref[r:r + sub, :], yft_ref[...])
        if r > 0:
            for cols in _columns(tokens):
                _stats(r - sub, sub, cols, first_row, log_ref, tgt_ref, m_ref, s_ref, tl_ref)


def _logits_kernel(tokens, last, rest, base_ref, emb_ref, yft_ref, tgt_ref, log_ref, m_ref, s_ref, tl_ref):
    tile = base_ref[0] + pl.program_id(0)

    @pl.when(pl.program_id(0) == 0)
    def _():
        m_ref[...] = jnp.full_like(m_ref, NEG)
        s_ref[...] = jnp.zeros_like(s_ref)
        tl_ref[...] = jnp.zeros_like(tl_ref)

    body = functools.partial(_logits_body, tokens=tokens, first_row=tile * TILE, emb_ref=emb_ref, yft_ref=yft_ref, tgt_ref=tgt_ref,
                             log_ref=log_ref, m_ref=m_ref, s_ref=s_ref, tl_ref=tl_ref)
    pl.when(tile != last)(lambda: body(TILE))
    pl.when(tile == last)(lambda: body(rest))


def _grad_columns(r, sub, cols, first_row, log_ref, vec_ref, tgt_ref, g_ref):
    log_z, scale, weight = vec_ref[0:1, cols], vec_ref[1:2, cols], vec_ref[2:3, cols]
    ids = tgt_ref[0:1, cols] - (first_row + r)
    step = min(sub, 64)
    row = lax.broadcasted_iota(jnp.int32, (step, LANES), 0)
    for k in range(0, sub, step):
        prob = jnp.exp(log_ref[r + k:r + k + step, cols] - log_z)
        grad = prob * scale - jnp.where(row == ids - k, weight, 0.0)
        g_ref[r + k:r + k + step, cols] = grad.astype(BF16)


def _emb_grad(r, sub, width, jobs, yf_ref, g_ref, de_refs):
    spans = range(0, width, SPAN)
    for n, c in enumerate(spans):
        part = _dot(g_ref[r:r + sub, :], yf_ref[:, c:c + SPAN])
        for de_ref in de_refs:
            de_ref[r:r + sub, c:c + SPAN] = part
        for job in jobs[n::len(spans)]:
            job()


def _column_jobs(r, rows, sub, tokens, *args):
    return [functools.partial(_grad_columns, r, sub, cols, *args) for cols in _columns(tokens)] if r < rows else []


def _own_body(rows, tokens, first_row, log_ref, emb_ref, yf_ref, vec_ref, tgt_ref, de_refs, dyf_ref, g_ref):
    sub = min(rows, SUB)
    width = yf_ref.shape[1]
    jobs = lambda r: _column_jobs(r, rows, sub, tokens, first_row, log_ref, vec_ref, tgt_ref, g_ref)
    for job in jobs(0):
        job()
    for r in range(0, rows, sub):
        _emb_grad(r, sub, width, jobs(r + sub), yf_ref, g_ref, de_refs)
    for c in range(0, width, SUB):
        dyf_ref[c:c + SUB, :] += lax.dot_general(emb_ref[0:rows, c:c + SUB], g_ref[0:rows, :], (((0,), (0,)), ((), ())),
                                                 preferred_element_type=F32)


def _own_kernel(tokens, last, rest, first, base_ref, log_ref, emb_ref, yf_ref, vec_ref, tgt_ref, *refs):
    if first:
        de_ref, dyf_ref, copy_ref, g_ref = refs
        de_refs = [de_ref, copy_ref]
    else:
        _, before_ref, de_ref, dyf_ref, g_ref = refs
        de_refs = [de_ref]
    tile = base_ref[0] + pl.program_id(0)

    @pl.when(pl.program_id(0) == 0)
    def _():
        dyf_ref[...] = jnp.zeros_like(dyf_ref) if first else before_ref[...]

    body = functools.partial(_own_body, tokens=tokens, first_row=tile * TILE, log_ref=log_ref, emb_ref=emb_ref, yf_ref=yf_ref,
                             vec_ref=vec_ref, tgt_ref=tgt_ref, de_refs=de_refs, dyf_ref=dyf_ref, g_ref=g_ref)
    if first:
        body(TILE)
    else:
        pl.when(tile != last)(lambda: body(TILE))
        pl.when(tile == last)(lambda: body(rest))


def _peer_body(rows, tokens, first_row, emb_ref, yft_ref, yf_ref, vec_ref, tgt_ref, de_ref, g_ref, log_ref):
    sub = min(rows, SUB)
    jobs = lambda r: _column_jobs(r, rows, sub, tokens, first_row, log_ref, vec_ref, tgt_ref, g_ref)

    def logits(r):
        if r < rows:
            log_ref[r:r + sub, :] = _dot(emb_ref[r:r + sub, :], yft_ref[...])

    logits(0)
    logits(sub)
    for job in jobs(0):
        job()
    for r in range(0, rows, sub):
        logits(r + 2 * sub)
        _emb_grad(r, sub, yf_ref.shape[1], jobs(r + sub), yf_ref, g_ref, [de_ref])


def _peer_kernel(tokens, last, rest, sent, pieces, base_ref, emb_ref, got_ref, yft_ref, yf_ref, vec_ref, tgt_ref, _, out_ref,
                 g_ref, log_ref, de_ref, sems):
    i = pl.program_id(0)
    slot = i % 2
    tile = base_ref[0] + sent + i
    body = functools.partial(_peer_body, tokens=tokens, first_row=tile * TILE, emb_ref=emb_ref, yft_ref=yft_ref, yf_ref=yf_ref,
                             vec_ref=vec_ref, tgt_ref=tgt_ref, de_ref=de_ref.at[slot], g_ref=g_ref, log_ref=log_ref)

    def store(which, rows, start=0):
        return pltpu.make_async_copy(de_ref.at[which, pl.ds(0, rows)], out_ref.at[pl.ds(start, rows)], sems.at[which])

    size = got_ref.shape[0]
    piece = pltpu.make_async_copy(got_ref, out_ref.at[pl.ds(base_ref[0] * TILE + jnp.minimum(i, pieces - 1) * size, size)], sems.at[2])
    pl.when(i < pieces)(lambda: piece.start())
    pl.when(i >= 2)(lambda: store(slot, TILE).wait())

    @pl.when(tile != last)
    def _():
        body(TILE)
        store(slot, TILE, tile * TILE).start()

    @pl.when(tile == last)
    def _():
        body(rest)
        store(slot, rest, tile * TILE).start()
        store(slot, rest).wait()

    pl.when(i < pieces)(lambda: piece.wait())

    @pl.when(i == pl.num_programs(0) - 1)
    def _():
        store(1 - slot, TILE).wait()
        pl.when(tile != last)(lambda: store(slot, TILE).wait())


def solution(mesh):
    def local_step(hidden, gain, emb_rows, targets, weights):
        vocab_rows, width = emb_rows.shape
        seq = hidden.shape[1]
        last, rest = vocab_rows // TILE, vocab_rows % TILE
        half = pl.cdiv(pl.cdiv(vocab_rows, TILE), 2)
        me = lax.axis_index('dp')
        swap = functools.partial(lax.ppermute, axis_name='dp', perm=[(0, 1), (1, 0)])

        hid_f32 = hidden[0].astype(F32)
        centered = hid_f32 - hid_f32.mean(-1, keepdims=True)
        inv_std = lax.rsqrt((centered * centered).mean(-1, keepdims=True) + LN_EPS)
        x_hat = centered * inv_std

        def both(mine, other):
            return jnp.where(me == 0, mine, other), jnp.where(me == 0, other, mine)

        x0, x1 = both(x_hat, swap(x_hat))
        t0, t1 = both(targets[0], swap(targets[0]))
        w0, w1 = both(weights[0], swap(weights[0]))
        n0 = w0.sum().astype(jnp.int32)
        n1 = w1.sum().astype(jnp.int32)
        blocks0, blocks1 = (n0 + BLOCK - 1) // BLOCK, (n1 + BLOCK - 1) // BLOCK
        start1 = blocks0 * BLOCK
        w_total = w0.sum() + w1.sum()

        def pack(a, b):
            zero = jnp.zeros_like(a)
            moved = lax.dynamic_slice(jnp.concatenate([zero, b, zero], 0), (seq - start1,) + (0,) * (a.ndim - 1), (2 * seq,) + a.shape[1:])
            first = lax.broadcasted_iota(jnp.int32, (2 * seq,) + (1,) * (a.ndim - 1), 0) < start1
            return jnp.where(first, jnp.concatenate([a, zero], 0), moved)

        yf = pack((x0 * gain).astype(BF16), (x1 * gain).astype(BF16))
        tok_scale = pack(w0, w1) / w_total
        local_ids = pack(t0, t1) - lax.axis_index('tp') * vocab_rows
        base_own = jnp.full((1,), half, jnp.int32) * me
        base_peer = jnp.full((1,), half, jnp.int32) * (1 - me)

        def branch(tokens):
            def run(yf, tok_scale, local_ids, emb_rows, base_own, base_peer):
                yf, tok_scale, local_ids = yf[:tokens], tok_scale[:tokens], local_ids[:tokens]
                yft = yf.T
                any_spec = pl.BlockSpec(memory_space=pl.ANY)
                one = pl.Buffered(1)
                row = lambda i, b: (b[0] + i, 0)
                near = lambda i, b: (i, 0)
                fixed = lambda i, b: (0, 0)
                emb_spec = pl.BlockSpec((TILE, width), row)
                yft_spec = pl.BlockSpec((width, tokens), fixed, pipeline_mode=one)
                yf_spec = pl.BlockSpec((tokens, width), fixed, pipeline_mode=one)
                log_spec = pl.BlockSpec((TILE, tokens), near)
                vec_spec = pl.BlockSpec((8, tokens), fixed)
                vec_shape = jax.ShapeDtypeStruct((8, tokens), F32)
                de_shape = jax.ShapeDtypeStruct((vocab_rows, width), F32)
                g_scratch = pltpu.VMEM((TILE, tokens), BF16)
                params = pltpu.CompilerParams(dimension_semantics=('arbitrary',), vmem_limit_bytes=62 * 2**20)

                sent, pieces = SENT[tokens // BLOCK]
                size = sent * TILE // pieces

                def call(kernel, name, dots, scalars, steps, ins, outs, shapes, scratch=(), args=(), **kw):
                    return pl.pallas_call(
                        functools.partial(kernel, tokens, last, rest, *args),
                        grid_spec=pltpu.PrefetchScalarGridSpec(num_scalar_prefetch=1, grid=(steps,), in_specs=ins, out_specs=outs,
                                                               scratch_shapes=scratch),
                        out_shape=shapes, compiler_params=params, name=name,
                        cost_estimate=pl.CostEstimate(flops=2 * dots * steps * TILE * tokens * width, transcendentals=0,
                                                      bytes_accessed=steps * TILE * (tokens + 2 * width) * 4), **kw)

                tgt = jnp.broadcast_to(local_ids[None], (8, tokens))
                logits, m, s, tl = call(_logits_kernel, 'logits', 1, base_own, half, [emb_spec, yft_spec, vec_spec],
                                        [log_spec, vec_spec, vec_spec, vec_spec],
                                        [jax.ShapeDtypeStruct((half * TILE, tokens), F32), vec_shape, vec_shape, vec_shape])(
                                            base_own, emb_rows, yft, tgt)
                m_dev = m.max(0)
                s_dev = (s * jnp.exp(m - m_dev[None])).sum(0)
                stats = lax.all_gather(jnp.stack([m_dev, s_dev, tl.sum(0)]), ('tp', 'dp'))
                peak = stats[:, 0].max(0)
                log_z = peak + jnp.log((stats[:, 1] * jnp.exp(stats[:, 0] - peak[None])).sum(0))
                loss = (tok_scale * (log_z - stats[:, 2].sum(0) + Z_COEF * log_z * log_z)).sum()
                vec = jnp.stack([log_z, (1.0 + 2.0 * Z_COEF * log_z) * tok_scale, tok_scale] + [tok_scale] * 5)

                dyf_spec = pl.BlockSpec((width, tokens), fixed, pipeline_mode=one)
                dyf_shape = jax.ShapeDtypeStruct((width, tokens), F32)
                later_spec = pl.BlockSpec((TILE, tokens), lambda i, b: (sent + i, 0))
                own_ins = [emb_spec, yf_spec, vec_spec, vec_spec]
                d_emb, dyf_a, send = call(_own_kernel, 'grads_first', 2, base_own, sent, [log_spec] + own_ins,
                                          [emb_spec, dyf_spec, pl.BlockSpec((TILE, width), near)],
                                          [de_shape, dyf_shape, jax.ShapeDtypeStruct((sent * TILE, width), F32)],
                                          [g_scratch], (True,))(base_own, logits, emb_rows, yf, vec, tgt)
                got = swap(send)
                d_emb, dyf_b = call(_own_kernel, 'grads_own', 2, base_own, half - sent, [later_spec] + own_ins + [any_spec, dyf_spec],
                                    [emb_spec, dyf_spec], [de_shape, dyf_shape], [g_scratch], (False,),
                                    input_output_aliases={6: 0})(base_own + sent, logits, emb_rows, yf, vec, tgt, d_emb, dyf_a)
                d_part = dyf_b.T
                d0 = d_part[:seq]
                d1 = lax.dynamic_slice(jnp.pad(d_part, ((0, 2 * seq - tokens), (0, 0))), (start1, 0), (seq, width))
                d_sum = lax.psum(jnp.where(me == 0, d0, d1) + swap(jnp.where(me == 0, d1, d0)), 'tp')
                d_emb = call(_peer_kernel, 'grads_peer', 2, base_peer, half - sent,
                             [pl.BlockSpec((TILE, width), lambda i, b: (b[0] + sent + i, 0)),
                              pl.BlockSpec((size, width), lambda i, b: (jnp.minimum(i, pieces - 1), 0)),
                              yft_spec, yf_spec, vec_spec, vec_spec, any_spec],
                             any_spec, de_shape,
                             [g_scratch, pltpu.VMEM((TILE, tokens), F32), pltpu.VMEM((2, TILE, width), F32), pltpu.SemaphoreType.DMA((3,))],
                             (sent, pieces), input_output_aliases={7: 0})(base_peer, emb_rows, got, yft, yf, vec, tgt, d_emb)
                d_emb, d_sum = lax.optimization_barrier((d_emb, d_sum))
                return d_emb, d_sum, loss
            return run

        sizes = range(5 * BLOCK, 2 * seq + 1, BLOCK)
        which = jnp.clip(blocks0 + blocks1 - 5, 0, len(sizes) - 1)
        d_emb, d_normed, loss = lax.switch(which, [branch(n) for n in sizes], yf, tok_scale, local_ids, emb_rows, base_own, base_peer)

        d_normed = jnp.where(weights[0][:, None] > 0, d_normed, 0.0)
        d_gain = (d_normed * x_hat).sum(0)
        d_gain = d_gain + swap(d_gain)
        d_rows = d_normed * gain
        d_hidden = inv_std * (d_rows - d_rows.mean(-1, keepdims=True) - x_hat * (d_rows * x_hat).mean(-1, keepdims=True))
        return loss, d_hidden.astype(BF16)[None], d_emb, d_gain

    return jax.shard_map(local_step, mesh=mesh,
                         in_specs=(P('dp', None, None), P(None), P('tp', None), P('dp', None), P('dp', None)),
                         out_specs=(P(), P('dp', None, None), P('tp', None), P(None)),
                         check_vma=False)
```
